32 devices in a mesh: kpt: 2 (over x), grid: 16 (over z, y, core).
Axes of the slice: x: 2, y: 2, z: 4, core: 2. Of those that a mesh axis runs over, the one named last changes fastest.
Arguments:
- orbitals: bfloat16 [4, 2, 2, 512, 256, 256], P('kpt', None, None, 'grid'), may hold values from -6 to 6
- kweights: int32 [4], P('kpt'), may hold values from 1 to 16
- occupations: int32 [4, 2], P('kpt'), may hold values from 0 to 2
- z_basis: float32 [512, 512], replicated, may hold values from -0.25 to 0.25
- z_eigen: float32 [512], replicated, may hold values from 0.25 to 4
Outputs:
- potential: float32 [512, 256, 256], P('grid')
The draws below stay inside these ranges and needn't reach their ends.
All inputs are finite; a program needn't handle non-finite values.
Results may differ from the reference program's by a relative error of at most 0.0003.
Values sent between devices are 32-bit elements; how exact they have to be, the bound alone decides.
A program may use at most 128 MiB of HBM per device.

```python
import math
import jax
import jax.numpy as jnp
from jax import lax

NX = 256
NY = 256
NZ = 512
KPD = 2
BANDS = 2
KPOINTS = 4


def draw_kweights(key, part):
    first, second = jax.random.split(jax.random.fold_in(key, 11))
    base = jax.random.randint(first, (KPOINTS,), 1, 17)
    chosen = jax.random.randint(second, (), 0, KPOINTS)
    places = jnp.arange(KPOINTS, dtype=jnp.int32)
    return jnp.where(places == chosen, 16, base).astype(jnp.int32)


def draw_occupations(key, part):
    first, second = jax.random.split(jax.random.fold_in(key, 23))
    base = jax.random.randint(first, (KPOINTS * BANDS,), 0, 3)
    order = jax.random.permutation(second, KPOINTS * BANDS)
    mixed = jnp.where(order == 0, 0, jnp.where(order == 1, 2, base))
    return mixed.reshape(KPOINTS, BANDS).astype(jnp.int32)


def block_scale(own_key, extent, shards, low, top_value):
    def one(position, blocks):
        steps = jax.random.uniform(jax.random.fold_in(jax.random.fold_in(own_key, 6), position), (blocks,), jnp.float32, low / len(shards), top_value / len(shards))
        return jnp.repeat(jnp.exp(steps), extent[position] // blocks).reshape((-1,) + (1,) * (len(extent) - position - 1))

    loudness = one(*shards[0])
    for cut in shards[1:]:
        loudness = loudness * one(*cut)
    return loudness


def scatter_about(own_key, extent, scale, most, cuts=(), held_as=jnp.bfloat16):
    level = block_scale(own_key, extent, cuts, -0.22, 0.18) if cuts else 1.0
    values = jax.random.normal(own_key, extent, jnp.float32) * scale * level
    return jnp.minimum(jnp.maximum(values, -most), most).astype(held_as)


def setup_inputs(seed: int = 0) -> dict:
    keys = jax.random.split(jax.random.key(seed), 6)
    orbitals = scatter_about(keys[0], (KPOINTS, BANDS, 2, NZ, NX, NY), 1.0, 6.0, ((0, 2), (3, 16)))
    kweights = draw_kweights(jax.random.fold_in(keys[5], 71), 0)
    occupations = draw_occupations(jax.random.fold_in(keys[5], 71), 0)
    z_basis = scatter_about(keys[3], (NZ, NZ), NZ ** -0.5, 0.25, (), jnp.float32)
    z_eigen = jnp.clip(jnp.exp(jax.random.uniform(keys[4], (NZ,), jnp.float32, math.log(0.25), math.log(4.0))), 0.25, 4.0)
    return {"orbitals": orbitals, "kweights": kweights, "occupations": occupations, "z_basis": z_basis, "z_eigen": z_eigen}


precise = lax.Precision.HIGHEST


def reference(orbitals, kweights, occupations, z_basis, z_eigen):
    factor = (kweights[:, None] * occupations).astype(jnp.float32) / (16.0 * KPD * BANDS)

    def add_point(kpoint, running):
        values = lax.dynamic_index_in_dim(orbitals, kpoint, 0, keepdims=False).astype(jnp.float32)
        weights = lax.dynamic_index_in_dim(factor, kpoint, 0, keepdims=False)
        return running + jnp.sum(weights[:, None, None, None, None] * values * values, axis=(0, 1))

    density = lax.fori_loop(0, KPOINTS, add_point, jnp.zeros((NZ, NX, NY), jnp.float32))
    spectrum = jnp.fft.fft2(density, axes=(1, 2))
    stacked = jnp.stack([jnp.real(spectrum), jnp.imag(spectrum)]).astype(jnp.float32)
    wave_x = jnp.arange(NX).astype(jnp.float32)
    wave_y = jnp.arange(NY).astype(jnp.float32)
    shift_x = 2.0 * jnp.sin(jnp.pi * wave_x / NX)
    shift_y = 2.0 * jnp.sin(jnp.pi * wave_y / NY)
    shifted = shift_x[:, None] ** 2 + shift_y[None, :] ** 2
    factors = 1.0 / (z_eigen[:, None, None] + shifted[None])
    projected = jnp.einsum('zj,czab->cjab', z_basis, stacked, precision=precise)
    filtered = jnp.einsum('zj,cjab->czab', z_basis, projected * factors[None], precision=precise)
    potential = jnp.fft.ifft2(lax.complex(filtered[0], filtered[1]), axes=(1, 2))
    return jnp.real(potential).astype(jnp.float32)
```

```python
import jax
import jax.numpy as jnp
from jax import lax
from jax.sharding import PartitionSpec as P


precise = lax.Precision.HIGH
CHUNKS = 4


def real_basis(length):
    position = jnp.arange(length, dtype=jnp.int32)
    product = position[:, None] * position[None, :] % length
    angles = product.astype(jnp.float32) * (2.0 * jnp.pi / length)
    lower = position[:, None] <= length // 2
    table = jnp.where(lower, jnp.cos(angles), jnp.sin(angles))
    edges = (position == 0) | (position == length // 2)
    weights = jnp.where(edges, 1.0, 2.0).astype(jnp.float32) / length
    return (table, table * weights[:, None])


def on_device(orbitals, kweights, occupations, z_basis, z_eigen):
    points, band_count, _, planes, x_length, y_length = orbitals.shape
    z_length = z_basis.shape[0]
    groups = lax.axis_size("kpt")
    blocks = lax.axis_size("grid")
    group = lax.axis_index("kpt")
    ky_count = y_length // groups
    kx_count = x_length // blocks
    step = max(planes // CHUNKS, 1)
    chunks = planes // step
    factor = (kweights[:, None] * occupations).astype(jnp.float32) / (16.0 * points * band_count)
    table_x, scaled_x = real_basis(x_length)
    table_y, scaled_y = real_basis(y_length)

    def part_of(table, shift):
        start = lax.rem(group + shift, groups) * ky_count
        return lax.dynamic_slice_in_dim(table, start, ky_count, 0)

    def shifted_by(shift):
        return [(g, (g + shift) % groups) for g in range(groups)]

    forward_y = [part_of(table_y, shift) for shift in range(groups)]
    inverse_y = [part_of(scaled_y, shift) for shift in range(groups)]
    basis = z_basis.reshape(blocks, planes, z_length)

    projected = None
    for chunk in range(chunks):
        rows = slice(chunk * step, (chunk + 1) * step)
        values = orbitals[:, :, :, rows].astype(jnp.float32)
        density = jnp.sum(factor[:, :, None, None, None, None] * values * values, axis=(0, 1, 2))
        along = jnp.einsum("zxy,ky->zxk", density, forward_y[0], precision=precise)
        for shift in range(1, groups):
            other = jnp.einsum("zxy,ky->zxk", density, forward_y[shift], precision=precise)
            arrived = lax.ppermute(other, "kpt", shifted_by(shift))
            along = along + arrived
        spectrum = jnp.einsum("jx,zxk->zjk", table_x, along, precision=precise)
        column = lax.all_to_all(
            spectrum.reshape(step, blocks, kx_count, ky_count), "grid", split_axis=1, concat_axis=0, tiled=True
        ).reshape(blocks * step, kx_count, ky_count)
        z_rows = basis[:, rows].reshape(blocks * step, z_length)
        term = jnp.einsum("zj,zab->jab", z_rows, column, precision=precise)
        projected = term if projected is None else projected + term

    wave_x = (lax.axis_index("grid") * kx_count + jnp.arange(kx_count, dtype=jnp.int32)).astype(jnp.float32)
    wave_y = (group * ky_count + jnp.arange(ky_count, dtype=jnp.int32)).astype(jnp.float32)
    shift_x = 2.0 * jnp.sin(jnp.pi * wave_x / x_length)
    shift_y = 2.0 * jnp.sin(jnp.pi * wave_y / y_length)
    shifted = shift_x[:, None] ** 2 + shift_y[None, :] ** 2
    scaled = projected * (1.0 / (z_eigen[:, None, None] + shifted[None]))

    outputs = []
    for chunk in range(chunks):
        rows = slice(chunk * step, (chunk + 1) * step)
        z_rows = basis[:, rows].reshape(blocks * step, z_length)
        filtered = jnp.einsum("zj,jab->zab", z_rows, scaled, precision=precise)
        modes = lax.all_to_all(
            filtered.reshape(blocks, step, kx_count, ky_count), "grid", split_axis=0, concat_axis=0, tiled=True
        )
        half = jnp.einsum(
            "jx,zjk->zxk",
            scaled_x,
            modes.transpose(1, 0, 2, 3).reshape(step, x_length, ky_count),
            precision=precise,
        )
        total = jnp.einsum("zxk,ky->zxy", half, inverse_y[0], precision=precise)
        for shift in range(1, groups):
            arrived = lax.ppermute(half, "kpt", shifted_by(groups - shift))
            total = total + jnp.einsum("zxk,ky->zxy", arrived, inverse_y[shift], precision=precise)
        outputs.append(total)
    return jnp.concatenate(outputs, axis=0)


def solution(mesh):
    return jax.shard_map(
        on_device,
        mesh=mesh,
        in_specs=(P("kpt", None, None, "grid", None, None), P("kpt"), P("kpt", None), P(), P()),
        out_specs=P("grid", None, None),
        check_vma=False,
    )
```
